32 devices in a mesh: beam: 2 (over x), pulse: 16 (over z, y, core).
Axes of the slice: x: 2, y: 2, z: 4, core: 2. Of those that a mesh axis runs over, the one named last changes fastest.
Arguments:
- echoes: float32 [2, 4096, 1536], P(None, 'pulse', 'beam'), parts along dimension 2, may hold values from -6 to 6
- guard_gates: int32 [1], replicated, may hold values from 1 to 4
- train_gates: int32 [1], replicated, may hold values from 4 to 16
Outputs:
- powers: float32 [4096, 1536], P('pulse', 'beam'), parts along dimension 1
- statistic: float32 [4096, 1536], P('pulse', 'beam'), parts along dimension 1
The draws below stay inside these ranges and needn't reach their ends.
There are 2 independent parts, one for each index of `beam`. The reference program is written for one: setup_inputs(seed, part) draws one part's arguments, and reference() takes and returns one part's arrays. A program takes and returns all parts, laid end to end along the dimension named above; an argument that names none is the same for every part. Nothing has to cross between parts.
All inputs are finite; a program needn't handle non-finite values.
Results may differ from the reference program's by a relative error of at most 0.0003.
Values sent between devices are 32-bit elements; how exact they have to be, the bound alone decides.
A program may use at most 192 MiB of HBM per device.

```python
import jax
import jax.numpy as jnp
from jax import lax

PULSES = 4096
GATES = 768
GUARD_BINS = 2
TRAIN_BINS = 4


def block_scale(rng, dims, split, smallest, largest):
    level, own = 1.0, jax.random.fold_in(rng, 6)
    for dim, shards_of in split:
        steps = jnp.exp(jax.random.uniform(jax.random.fold_in(own, dim), (shards_of,), jnp.float32, smallest / len(split), largest / len(split)))
        level = level * jnp.repeat(steps, dims[dim] // shards_of).reshape([-1 if axis == dim else 1 for axis in range(len(dims))])
    return level


def centred(rng, dims, scale, limit, pieces=(), kind=jnp.bfloat16):
    array = jax.random.normal(rng, dims, jnp.float32) * scale
    if len(pieces) > 0:
        array = block_scale(rng, dims, pieces, -0.22, 0.18) * array
    return jnp.clip(array, min=-limit, max=limit).astype(kind)


def setup_inputs(seed: int = 0, part: int = 0) -> dict:
    keys = jax.random.split(jax.random.key(seed), 4)
    part_splits = jax.random.split(jax.random.fold_in(keys[3], part), 4)
    return {
        "echoes": centred(part_splits[0], (2, PULSES, GATES), 1.0, 6.0, ((1, 16),), jnp.float32),
        "guard_gates": jax.random.randint(keys[1], (1,), 1, 5).astype(jnp.int32),
        "train_gates": jax.random.randint(keys[2], (1,), 4, 17).astype(jnp.int32),
    }


TWO_PI = 6.283185307179586

def tables(bin_first, bin_count, pulse_first, pulse_count):
    bin_ids = bin_first + jnp.arange(bin_count, dtype=jnp.int32)
    pulse_ids = pulse_first + jnp.arange(pulse_count, dtype=jnp.int32)
    phases = (bin_ids[:, None] * pulse_ids[None, :] % PULSES).astype(jnp.float32) * (TWO_PI / PULSES)
    return (jnp.cos(phases), jnp.sin(phases))

def transform(cosine, sine, samples):
    width = samples.shape[2]
    stacked = jnp.concatenate([samples[0], samples[1]], axis=1)
    first_part = jnp.dot(cosine, stacked, precision=lax.Precision.HIGHEST, preferred_element_type=jnp.float32)
    second_part = jnp.dot(sine, stacked, precision=lax.Precision.HIGHEST, preferred_element_type=jnp.float32)
    real_part = first_part[:, :width] + second_part[:, width:]
    imag_part = first_part[:, width:] - second_part[:, :width]
    return (real_part, imag_part)

def reference(echoes, guard_gates, train_gates):
    scale_factor = 1.0 / jnp.sqrt(jnp.float32(PULSES))

    def one_block(bin_first):
        cosine, sine = tables(bin_first, 512, 0, PULSES)
        real_part, imag_part = transform(cosine, sine, echoes)
        real_part = real_part * scale_factor
        imag_part = imag_part * scale_factor
        return real_part * real_part + imag_part * imag_part
    starts = jnp.arange(PULSES // 512, dtype=jnp.int32) * 512
    powers = lax.map(one_block, starts).reshape(PULSES, GATES)
    guard_width = guard_gates[0]
    train_width = train_gates[0]
    gate_ids = jnp.arange(GATES, dtype=jnp.int32)
    offsets = jnp.abs(gate_ids[:, None] - gate_ids[None, :])
    band = ((offsets > guard_width) & (offsets <= guard_width + train_width)).astype(jnp.float32)
    range_sum = jnp.dot(powers, band, precision=lax.Precision.HIGHEST, preferred_element_type=jnp.float32)
    range_count = lax.optimization_barrier(jnp.sum(band, axis=0))
    doppler_sum = jnp.zeros_like(powers)
    for shift_bins in range(GUARD_BINS + 1, GUARD_BINS + TRAIN_BINS + 1):
        doppler_sum = doppler_sum + jnp.roll(powers, -shift_bins, axis=0) + jnp.roll(powers, shift_bins, axis=0)
    noise_level = (range_sum + doppler_sum) / (range_count[None, :] + 2.0 * TRAIN_BINS)
    statistic = powers / (noise_level + 1.0)
    return (powers, statistic)
```

```python
import functools

import jax
import jax.numpy as jnp
import numpy as np
from jax import lax
from jax.experimental import pallas as pl
from jax.experimental.pallas import tpu as pltpu
from jax.sharding import PartitionSpec as P

PULSES = 4096
GUARD_BINS = 2
TRAIN_BINS = 4


TWO_PI = 6.283185307179586


def padded_2(cells, sides, width):
    for axis, dim in sides:
        count = lax.axis_size(axis)
        head = lax.slice_in_dim(cells, 0, width, axis=dim)
        tail = lax.slice_in_dim(cells, cells.shape[dim] - width, cells.shape[dim], axis=dim)
        cells = jnp.concatenate(
            [
                lax.ppermute(tail, axis, [(i, (i + 1) % count) for i in range(count)]),
                cells,
                lax.ppermute(head, axis, [((i + 1) % count, i) for i in range(count)]),
            ],
            axis=dim,
        )
    return cells


def small_tables(count):
    index_row = jnp.arange(count, dtype=jnp.int32)
    phases = (index_row[:, None] * index_row[None, :] % count).astype(jnp.float32) * (
        TWO_PI / count
    )
    return (jnp.cos(phases), jnp.sin(phases))


def product(left, right):
    return jnp.dot(left, right, precision=lax.Precision.HIGHEST, preferred_element_type=jnp.float32)


def factored_powers(samples):
    width = samples.shape[2]
    bit_count = PULSES.bit_length() - 1
    first_radix = 2 ** (bit_count // 2)
    second_radix = PULSES // first_radix
    cos_first, sin_first = small_tables(first_radix)
    real_in = samples[0].reshape(first_radix, second_radix * width)
    imag_in = samples[1].reshape(first_radix, second_radix * width)
    real_one = (product(cos_first, real_in) + product(sin_first, imag_in)).reshape(
        first_radix, second_radix, width
    )
    imag_one = (product(cos_first, imag_in) - product(sin_first, real_in)).reshape(
        first_radix, second_radix, width
    )
    first_ids = jnp.arange(first_radix, dtype=jnp.int32)
    second_ids = jnp.arange(second_radix, dtype=jnp.int32)
    twist = (first_ids[:, None] * second_ids[None, :] % PULSES).astype(jnp.float32) * (
        TWO_PI / PULSES
    )
    twist_cos = jnp.cos(twist)[:, :, None]
    twist_sin = jnp.sin(twist)[:, :, None]
    real_two = twist_cos * real_one + twist_sin * imag_one
    imag_two = twist_cos * imag_one - twist_sin * real_one
    real_two = jnp.transpose(real_two, (1, 0, 2)).reshape(second_radix, first_radix * width)
    imag_two = jnp.transpose(imag_two, (1, 0, 2)).reshape(second_radix, first_radix * width)
    cos_second, sin_second = small_tables(second_radix)
    scale_factor = 1.0 / jnp.sqrt(jnp.float32(PULSES))
    real_out = (product(cos_second, real_two) + product(sin_second, imag_two)) * scale_factor
    imag_out = (product(cos_second, imag_two) - product(sin_second, real_two)) * scale_factor
    result = real_out * real_out + imag_out * imag_out
    return result.reshape(PULSES, width)


def generic_shards(echoes, guard_gates, train_gates):
    devices_count = lax.axis_size("pulse")
    bins_local = PULSES // devices_count
    gates_count = echoes.shape[2]
    columns = factored_powers(
        lax.all_to_all(echoes, "pulse", split_axis=2, concat_axis=1, tiled=True)
    )
    powers = lax.all_to_all(columns, "pulse", split_axis=0, concat_axis=1, tiled=True)
    reach = GUARD_BINS + TRAIN_BINS
    padded = padded_2(powers, (("pulse", 0),), reach)
    doppler_sum = jnp.zeros_like(powers)
    for shift_bins in range(GUARD_BINS + 1, reach + 1):
        above = padded[reach + shift_bins : reach + shift_bins + bins_local]
        below = padded[reach - shift_bins : reach - shift_bins + bins_local]
        doppler_sum = doppler_sum + above + below
    guard_width = guard_gates[0]
    train_width = train_gates[0]
    gate_ids = jnp.arange(gates_count, dtype=jnp.int32)
    offsets = jnp.abs(gate_ids[:, None] - gate_ids[None, :])
    band = ((offsets > guard_width) & (offsets <= guard_width + train_width)).astype(jnp.float32)
    range_sum = jnp.dot(
        powers, band, precision=lax.Precision.HIGHEST, preferred_element_type=jnp.float32
    )
    range_count = jnp.sum(band, axis=0)
    noise_level = (range_sum + doppler_sum) / (range_count[None, :] + 2.0 * TRAIN_BINS)
    statistic = powers / (noise_level + 1.0)
    return (powers, statistic)


LANES = 128
ROWS = 8
HIGHEST = lax.Precision.HIGHEST


def butterflies(cells):
    count = len(cells)
    if count == 1:
        return cells
    even = butterflies(cells[0::2])
    odd = butterflies(cells[1::2])
    low, high = [], []
    for k in range(count // 2):
        re, im = odd[k]
        if 4 * k == count:
            re, im = im, -re
        elif k:
            c, s = np.cos(2 * np.pi * k / count), np.sin(2 * np.pi * k / count)
            c, s = np.float32(c), np.float32(s)
            re, im = c * re + s * im, c * im - s * re
        low.append((even[k][0] + re, even[k][1] + im))
        high.append((even[k][0] - re, even[k][1] - im))
    return low + high


def swap_digits(rows, width):
    count = len(rows)
    lane = lax.broadcasted_iota(jnp.int32, rows[0][0].shape, 1)
    bit = 1
    while bit < count:
        step = bit * width
        keep = (lane // step) % 2 == 0 if step < LANES else None
        for f in range(count):
            if f & bit:
                continue
            first, second = rows[f], rows[f | bit]
            if step < LANES:
                new_first = [
                    jnp.where(keep, a, pltpu.roll(b, step, 1)) for a, b in zip(first, second)
                ]
                new_second = [
                    jnp.where(keep, pltpu.roll(a, LANES - step, 1), b)
                    for a, b in zip(first, second)
                ]
            else:
                hop = step // LANES
                new_first, new_second = list(first), list(second)
                for h in range(len(first)):
                    if h & hop:
                        new_first[h] = second[h ^ hop]
                    else:
                        new_second[h] = first[h ^ hop]
            rows[f], rows[f | bit] = new_first, new_second
        bit *= 2
    return rows


def split(values):
    high = values.astype(jnp.bfloat16)
    return high, (values - high.astype(jnp.float32)).astype(jnp.bfloat16)


def bf16_dot(left, right, dims=(((1,), (0,)), ((), ()))):
    return lax.dot_general(left, right, dims, preferred_element_type=jnp.float32)


def kernel(
    n, chunks, guard_ref, train_ref, x_ref, table_high, table_low, twist_cos, twist_sin, perm_ref,
    power_ref, stat_ref,
    sent, got, mixed, cells, landed, padded, edges,
    send_one, recv_one, send_two, recv_two, send_edge, recv_edge,
):
    me = lax.axis_index("pulse")
    length, gates = x_ref.shape[1], x_ref.shape[2]
    part = gates // n // chunks
    halves = length // LANES
    barrier = pltpu.get_barrier_semaphore()
    for o in range(1, n):
        pl.semaphore_signal(barrier, inc=1, device_id={"pulse": lax.rem(me + o, n)})
    for p in range(2):
        sent[:, :, p] = x_ref[p].T.reshape(n, chunks, part, length)
    pl.semaphore_wait(barrier, n - 1)

    def first_copy(c, o):
        peer = lax.rem(me + o, n)
        return pltpu.make_async_remote_copy(
            src_ref=sent.at[peer, c], dst_ref=got.at[c, me],
            send_sem=send_one.at[c, o], recv_sem=recv_one.at[c, o],
            device_id={"pulse": peer},
        )

    def second_copy(c, o):
        peer = lax.rem(me + o, n)
        return pltpu.make_async_remote_copy(
            src_ref=cells.at[peer, c], dst_ref=landed.at[me, c],
            send_sem=send_two.at[c, o], recv_sem=recv_two.at[c, o],
            device_id={"pulse": peer},
        )

    order = peer_order(n)
    for c in range(chunks):
        for o in order:
            first_copy(c, o).start()
    for c in range(chunks):
        got[c, me] = sent[me, c]
    gate_row = lax.broadcasted_iota(jnp.int32, (gates, gates), 0)
    gate_col = lax.broadcasted_iota(jnp.int32, (gates, gates), 1)
    offsets = jnp.abs(gate_row - gate_col)
    guard, train = guard_ref[0], train_ref[0]
    inside = ((offsets > guard) & (offsets <= guard + train)).astype(jnp.float32)
    range_count = jnp.sum(inside, axis=0, keepdims=True)
    band = inside.astype(jnp.bfloat16)

    for c in range(chunks):
        for o in order:
            first_copy(c, o).wait_recv()
        for r in range(0, part, ROWS):
            for h in range(halves):
                lanes = slice(h * LANES, (h + 1) * LANES)
                spectra = butterflies(
                    [
                        (got[c, s, 0, r : r + ROWS, lanes], got[c, s, 1, r : r + ROWS, lanes])
                        for s in range(n)
                    ]
                )
                for f, (re, im) in enumerate(spectra):
                    tc, ts = twist_cos[f : f + 1, lanes], twist_sin[f : f + 1, lanes]
                    mixed[0, f, r : r + ROWS, lanes] = tc * re + ts * im
                    mixed[1, f, r : r + ROWS, lanes] = tc * im - ts * re
        high, low = split(mixed[...].reshape(2 * n * part, length))
        both = (
            bf16_dot(high, table_high[...])
            + bf16_dot(low, table_high[...])
            + bf16_dot(high, table_low[...])
        ).reshape(2, n * part, 2 * length)
        real = both[0, :, :length] + both[1, :, length:]
        imag = both[1, :, :length] - both[0, :, length:]
        power = (real * real + imag * imag).reshape(n, part, length)
        rows = [
            [power[f, :, h * LANES : (h + 1) * LANES] for h in range(halves)] for f in range(n)
        ]
        rows = swap_digits(rows, length // n)
        for d in range(n):
            for h in range(halves):
                cells[d, c, :, h * LANES : (h + 1) * LANES] = rows[d][h]
        for o in order:
            second_copy(c, o).start()
        landed[me, c] = cells[me, c]
    for c in range(chunks):
        for o in order:
            second_copy(c, o).wait_recv()

    columns = landed[...].reshape(gates, length)
    powers = lax.dot_general(
        perm_ref[...], columns, (((1,), (1,)), ((), ())),
        precision=HIGHEST, preferred_element_type=jnp.float32,
    )
    power_ref[...] = powers
    edges[0] = powers[:ROWS]
    edges[1] = powers[length - ROWS :]
    above, below = lax.rem(me + 1, n), lax.rem(me + n - 1, n)
    tail_copy = pltpu.make_async_remote_copy(
        src_ref=edges.at[1], dst_ref=edges.at[2],
        send_sem=send_edge.at[0], recv_sem=recv_edge.at[0], device_id={"pulse": above},
    )
    head_copy = pltpu.make_async_remote_copy(
        src_ref=edges.at[0], dst_ref=edges.at[3],
        send_sem=send_edge.at[1], recv_sem=recv_edge.at[1], device_id={"pulse": below},
    )
    tail_copy.start()
    head_copy.start()
    high, low = split(powers)
    range_sum = bf16_dot(high, band) + bf16_dot(low, band)
    padded[ROWS : ROWS + length] = powers
    tail_copy.wait_recv()
    head_copy.wait_recv()
    padded[:ROWS] = edges[2]
    padded[ROWS + length :] = edges[3]
    total = range_sum
    for d in range(GUARD_BINS + 1, GUARD_BINS + TRAIN_BINS + 1):
        total = total + padded[ROWS + d : ROWS + d + length] + padded[ROWS - d : ROWS - d + length]
    noise = total / (range_count + 2.0 * TRAIN_BINS)
    stat_ref[...] = powers / (noise + 1.0)
    tail_copy.wait_send()
    head_copy.wait_send()
    for c in range(chunks):
        for o in order:
            first_copy(c, o).wait_send()
            second_copy(c, o).wait_send()


def peer_order(n):
    return list(range(1, n))


def tables(n, length):
    lane = np.arange(length)
    turn = 2 * np.pi * (np.outer(lane, lane) % length) / length
    both = np.concatenate([np.cos(turn), np.sin(turn)], axis=1).astype(np.float32)
    high = both.astype(jnp.bfloat16)
    low = (both - high.astype(np.float32)).astype(jnp.bfloat16)
    twist = 2 * np.pi * np.outer(np.arange(n), lane) / (n * length)
    scale = 1.0 / np.sqrt(n * length)
    perm = np.zeros((length, length), np.float32)
    width = length // n
    for f in range(n):
        for e in range(width):
            perm[f + n * e, f * width + e] = 1.0
    return (
        high, low,
        (np.cos(twist) * scale).astype(np.float32),
        (np.sin(twist) * scale).astype(np.float32),
        perm,
    )


def kernel_shards(echoes, guard_gates, train_gates):
    n = lax.axis_size("pulse")
    length, gates = echoes.shape[1], echoes.shape[2]
    chunks = CHUNKS if gates % (n * ROWS * CHUNKS) == 0 else 1
    part = gates // n // chunks
    smem = pl.BlockSpec(memory_space=pltpu.SMEM)
    vmem = pl.BlockSpec(memory_space=pltpu.VMEM)
    out = jax.ShapeDtypeStruct((length, gates), jnp.float32)
    dma = pltpu.SemaphoreType.DMA
    return pl.pallas_call(
        functools.partial(kernel, n, chunks),
        out_shape=(out, out),
        in_specs=[smem, smem] + [vmem] * 6,
        out_specs=(vmem, vmem),
        scratch_shapes=[
            pltpu.VMEM((n, chunks, 2, part, length), jnp.float32),
            pltpu.VMEM((chunks, n, 2, part, length), jnp.float32),
            pltpu.VMEM((2, n, part, length), jnp.float32),
            pltpu.VMEM((n, chunks, part, length), jnp.float32),
            pltpu.VMEM((n, chunks, part, length), jnp.float32),
            pltpu.VMEM((length + 2 * ROWS, gates), jnp.float32),
            pltpu.VMEM((4, ROWS, gates), jnp.float32),
            dma((chunks, n)), dma((chunks, n)), dma((chunks, n)), dma((chunks, n)),
            dma((2,)), dma((2,)),
        ],
        compiler_params=pltpu.CompilerParams(
            collective_id=0, has_side_effects=True, vmem_limit_bytes=60 * 2**20
        ),
    )(guard_gates, train_gates, echoes, *(jnp.asarray(t) for t in tables(n, length)))


CHUNKS = 3


def shards(echoes, guard_gates, train_gates):
    n = lax.axis_size("pulse")
    length, gates = echoes.shape[1], echoes.shape[2]
    fits = length % LANES == 0 and length % n == 0 and n > 2 and gates % (n * ROWS) == 0
    fits = fits and n & (n - 1) == 0 and length & (length - 1) == 0 and LANES % (length // n) == 0
    if fits and GUARD_BINS + TRAIN_BINS <= ROWS:
        return kernel_shards(echoes, guard_gates, train_gates)
    return generic_shards(echoes, guard_gates, train_gates)


def solution(mesh):
    return jax.shard_map(
        shards,
        mesh=mesh,
        in_specs=(P(None, "pulse", "beam"), P(), P()),
        out_specs=(P("pulse", "beam"), P("pulse", "beam")),
        check_vma=False,
    )
```

```python
import functools

import jax
import jax.numpy as jnp
import numpy as np
from jax import lax
from jax.experimental import pallas as pl
from jax.experimental.pallas import tpu as pltpu
from jax.sharding import PartitionSpec as P

PULSES = 4096
GUARD_BINS = 2
TRAIN_BINS = 4


TWO_PI = 6.283185307179586


def padded_2(cells, sides, width):
    for axis, dim in sides:
        count = lax.axis_size(axis)
        head = lax.slice_in_dim(cells, 0, width, axis=dim)
        tail = lax.slice_in_dim(cells, cells.shape[dim] - width, cells.shape[dim], axis=dim)
        cells = jnp.concatenate(
            [
                lax.ppermute(tail, axis, [(i, (i + 1) % count) for i in range(count)]),
                cells,
                lax.ppermute(head, axis, [((i + 1) % count, i) for i in range(count)]),
            ],
            axis=dim,
        )
    return cells


def small_tables(count):
    index_row = jnp.arange(count, dtype=jnp.int32)
    phases = (index_row[:, None] * index_row[None, :] % count).astype(jnp.float32) * (
        TWO_PI / count
    )
    return (jnp.cos(phases), jnp.sin(phases))


def product(left, right):
    return jnp.dot(left, right, precision=lax.Precision.HIGHEST, preferred_element_type=jnp.float32)


def factored_powers(samples):
    width = samples.shape[2]
    bit_count = PULSES.bit_length() - 1
    first_radix = 2 ** (bit_count // 2)
    second_radix = PULSES // first_radix
    cos_first, sin_first = small_tables(first_radix)
    real_in = samples[0].reshape(first_radix, second_radix * width)
    imag_in = samples[1].reshape(first_radix, second_radix * width)
    real_one = (product(cos_first, real_in) + product(sin_first, imag_in)).reshape(
        first_radix, second_radix, width
    )
    imag_one = (product(cos_first, imag_in) - product(sin_first, real_in)).reshape(
        first_radix, second_radix, width
    )
    first_ids = jnp.arange(first_radix, dtype=jnp.int32)
    second_ids = jnp.arange(second_radix, dtype=jnp.int32)
    twist = (first_ids[:, None] * second_ids[None, :] % PULSES).astype(jnp.float32) * (
        TWO_PI / PULSES
    )
    twist_cos = jnp.cos(twist)[:, :, None]
    twist_sin = jnp.sin(twist)[:, :, None]
    real_two = twist_cos * real_one + twist_sin * imag_one
    imag_two = twist_cos * imag_one - twist_sin * real_one
    real_two = jnp.transpose(real_two, (1, 0, 2)).reshape(second_radix, first_radix * width)
    imag_two = jnp.transpose(imag_two, (1, 0, 2)).reshape(second_radix, first_radix * width)
    cos_second, sin_second = small_tables(second_radix)
    scale_factor = 1.0 / jnp.sqrt(jnp.float32(PULSES))
    real_out = (product(cos_second, real_two) + product(sin_second, imag_two)) * scale_factor
    imag_out = (product(cos_second, imag_two) - product(sin_second, real_two)) * scale_factor
    result = real_out * real_out + imag_out * imag_out
    return result.reshape(PULSES, width)


def generic_shards(echoes, guard_gates, train_gates):
    devices_count = lax.axis_size("pulse")
    bins_local = PULSES // devices_count
    gates_count = echoes.shape[2]
    columns = factored_powers(
        lax.all_to_all(echoes, "pulse", split_axis=2, concat_axis=1, tiled=True)
    )
    powers = lax.all_to_all(columns, "pulse", split_axis=0, concat_axis=1, tiled=True)
    reach = GUARD_BINS + TRAIN_BINS
    padded = padded_2(powers, (("pulse", 0),), reach)
    doppler_sum = jnp.zeros_like(powers)
    for shift_bins in range(GUARD_BINS + 1, reach + 1):
        above = padded[reach + shift_bins : reach + shift_bins + bins_local]
        below = padded[reach - shift_bins : reach - shift_bins + bins_local]
        doppler_sum = doppler_sum + above + below
    guard_width = guard_gates[0]
    train_width = train_gates[0]
    gate_ids = jnp.arange(gates_count, dtype=jnp.int32)
    offsets = jnp.abs(gate_ids[:, None] - gate_ids[None, :])
    band = ((offsets > guard_width) & (offsets <= guard_width + train_width)).astype(jnp.float32)
    range_sum = jnp.dot(
        powers, band, precision=lax.Precision.HIGHEST, preferred_element_type=jnp.float32
    )
    range_count = jnp.sum(band, axis=0)
    noise_level = (range_sum + doppler_sum) / (range_count[None, :] + 2.0 * TRAIN_BINS)
    statistic = powers / (noise_level + 1.0)
    return (powers, statistic)


LANES = 128
ROWS = 8
HIGHEST = lax.Precision.HIGHEST


def butterflies(cells):
    count = len(cells)
    if count == 1:
        return cells
    even = butterflies(cells[0::2])
    odd = butterflies(cells[1::2])
    low, high = [], []
    for k in range(count // 2):
        re, im = odd[k]
        if 4 * k == count:
            re, im = im, -re
        elif k:
            c, s = np.cos(2 * np.pi * k / count), np.sin(2 * np.pi * k / count)
            c, s = np.float32(c), np.float32(s)
            re, im = c * re + s * im, c * im - s * re
        low.append((even[k][0] + re, even[k][1] + im))
        high.append((even[k][0] - re, even[k][1] - im))
    return low + high


def swap_digits(rows, width):
    count = len(rows)
    lane = lax.broadcasted_iota(jnp.int32, rows[0][0].shape, 1)
    bit = 1
    while bit < count:
        step = bit * width
        keep = (lane // step) % 2 == 0 if step < LANES else None
        for f in range(count):
            if f & bit:
                continue
            first, second = rows[f], rows[f | bit]
            if step < LANES:
                new_first = [
                    jnp.where(keep, a, pltpu.roll(b, step, 1)) for a, b in zip(first, second)
                ]
                new_second = [
                    jnp.where(keep, pltpu.roll(a, LANES - step, 1), b)
                    for a, b in zip(first, second)
                ]
            else:
                hop = step // LANES
                new_first, new_second = list(first), list(second)
                for h in range(len(first)):
                    if h & hop:
                        new_first[h] = second[h ^ hop]
                    else:
                        new_second[h] = first[h ^ hop]
            rows[f], rows[f | bit] = new_first, new_second
        bit *= 2
    return rows


def split(values):
    high = values.astype(jnp.bfloat16)
    return high, (values - high.astype(jnp.float32)).astype(jnp.bfloat16)


def bf16_dot(left, right, dims=(((1,), (0,)), ((), ()))):
    return lax.dot_general(left, right, dims, preferred_element_type=jnp.float32)


def kernel(
    n, chunks, guard_ref, train_ref, x_any, high_any, low_any, cos_any, sin_any, perm_any,
    power_ref, stat_ref,
    sent, got, mixed, cells, landed, padded, edges,
    x_ref, table_high, table_low, twist_cos, twist_sin, perm_ref,
    send_one, recv_one, send_two, recv_two, send_edge, recv_edge, load,
):
    me = lax.axis_index("pulse")
    length, gates = x_ref.shape[1], x_ref.shape[2]
    part = gates // n // chunks
    halves = length // LANES
    barrier = pltpu.get_barrier_semaphore()
    for o in range(1, n):
        pl.semaphore_signal(barrier, inc=1, device_id={"pulse": lax.rem(me + o, n)})
    loads = [pltpu.make_async_copy(x_any.at[p], x_ref.at[p], load.at[p]) for p in range(2)]
    pairs = (
        (high_any, table_high), (low_any, table_low), (cos_any, twist_cos), (sin_any, twist_sin),
        (perm_any, perm_ref),
    )
    for i, (source, target) in enumerate(pairs):
        loads.append(pltpu.make_async_copy(source, target, load.at[2 + i]))
    for copy in loads:
        copy.start()
    for p in range(2):
        loads[p].wait()
        sent[:, :, p] = x_ref[p].T.reshape(n, chunks, part, length)
    pl.semaphore_wait(barrier, n - 1)

    def first_copy(c, o):
        peer = partner(me, o)
        return pltpu.make_async_remote_copy(
            src_ref=sent.at[peer, c], dst_ref=got.at[c, me],
            send_sem=send_one.at[c, o], recv_sem=recv_one.at[c, o],
            device_id={"pulse": peer},
        )

    def second_copy(c, o):
        peer = partner(me, o)
        return pltpu.make_async_remote_copy(
            src_ref=cells.at[peer, c], dst_ref=landed.at[me, c],
            send_sem=send_two.at[c, o], recv_sem=recv_two.at[c, o],
            device_id={"pulse": peer},
        )

    order = peer_order(n)
    for c in range(chunks):
        for o in order:
            first_copy(c, o).start()
    for c in range(chunks):
        got[c, me] = sent[me, c]
    for copy in loads[2:]:
        copy.wait()
    gate_row = lax.broadcasted_iota(jnp.int32, (gates, gates), 0)
    gate_col = lax.broadcasted_iota(jnp.int32, (gates, gates), 1)
    offsets = jnp.abs(gate_row - gate_col)
    guard, train = guard_ref[0], train_ref[0]
    inside = ((offsets > guard) & (offsets <= guard + train)).astype(jnp.float32)
    range_count = jnp.sum(inside, axis=0, keepdims=True)
    band = inside.astype(jnp.bfloat16)

    for c in range(chunks):
        for o in order:
            first_copy(c, o).wait_recv()
        for r in range(0, part, ROWS):
            for h in range(halves):
                lanes = slice(h * LANES, (h + 1) * LANES)
                spectra = butterflies(
                    [
                        (got[c, s, 0, r : r + ROWS, lanes], got[c, s, 1, r : r + ROWS, lanes])
                        for s in range(n)
                    ]
                )
                for f, (re, im) in enumerate(spectra):
                    tc, ts = twist_cos[f : f + 1, lanes], twist_sin[f : f + 1, lanes]
                    mixed[0, f, r : r + ROWS, lanes] = tc * re + ts * im
                    mixed[1, f, r : r + ROWS, lanes] = tc * im - ts * re
        high, low = split(mixed[...].reshape(2 * n * part, length))
        both = (
            bf16_dot(high, table_high[...])
            + bf16_dot(low, table_high[...])
            + bf16_dot(high, table_low[...])
        ).reshape(2, n * part, 2 * length)
        real = both[0, :, :length] + both[1, :, length:]
        imag = both[1, :, :length] - both[0, :, length:]
        power = (real * real + imag * imag).reshape(n, part, length)
        rows = [
            [power[f, :, h * LANES : (h + 1) * LANES] for h in range(halves)] for f in range(n)
        ]
        rows = swap_digits(rows, length // n)
        for d in range(n):
            for h in range(halves):
                cells[d, c, :, h * LANES : (h + 1) * LANES] = rows[d][h]
        for o in order:
            second_copy(c, o).start()
        landed[me, c] = cells[me, c]
    for c in range(chunks):
        for o in order:
            second_copy(c, o).wait_recv()

    columns = landed[...].reshape(gates, length)
    powers = lax.dot_general(
        perm_ref[...], columns, (((1,), (1,)), ((), ())),
        precision=HIGHEST, preferred_element_type=jnp.float32,
    )
    power_ref[...] = powers
    edges[0] = powers[:ROWS]
    edges[1] = powers[length - ROWS :]
    above, below = lax.rem(me + 1, n), lax.rem(me + n - 1, n)
    tail_copy = pltpu.make_async_remote_copy(
        src_ref=edges.at[1], dst_ref=edges.at[2],
        send_sem=send_edge.at[0], recv_sem=recv_edge.at[0], device_id={"pulse": above},
    )
    head_copy = pltpu.make_async_remote_copy(
        src_ref=edges.at[0], dst_ref=edges.at[3],
        send_sem=send_edge.at[1], recv_sem=recv_edge.at[1], device_id={"pulse": below},
    )
    tail_copy.start()
    head_copy.start()
    high, low = split(powers)
    range_sum = bf16_dot(high, band) + bf16_dot(low, band)
    padded[ROWS : ROWS + length] = powers
    tail_copy.wait_recv()
    head_copy.wait_recv()
    padded[:ROWS] = edges[2]
    padded[ROWS + length :] = edges[3]
    total = range_sum
    for d in range(GUARD_BINS + 1, GUARD_BINS + TRAIN_BINS + 1):
        total = total + padded[ROWS + d : ROWS + d + length] + padded[ROWS - d : ROWS - d + length]
    noise = total / (range_count + 2.0 * TRAIN_BINS)
    stat_ref[...] = powers / (noise + 1.0)
    tail_copy.wait_send()
    head_copy.wait_send()
    for c in range(chunks):
        for o in order:
            first_copy(c, o).wait_send()
            second_copy(c, o).wait_send()


def partner(me, offset):
    peer, bit = me, 1
    while bit <= offset:
        if offset & bit:
            peer = peer + bit * (1 - 2 * lax.rem(lax.div(me, bit), 2))
        bit *= 2
    return peer


def peer_order(n):
    return list(range(n - 1, 0, -1))


def tables(n, length):
    lane = np.arange(length)
    turn = 2 * np.pi * (np.outer(lane, lane) % length) / length
    both = np.concatenate([np.cos(turn), np.sin(turn)], axis=1).astype(np.float32)
    high = both.astype(jnp.bfloat16)
    low = (both - high.astype(np.float32)).astype(jnp.bfloat16)
    twist = 2 * np.pi * np.outer(np.arange(n), lane) / (n * length)
    scale = 1.0 / np.sqrt(n * length)
    perm = np.zeros((length, length), np.float32)
    width = length // n
    for f in range(n):
        for e in range(width):
            perm[f + n * e, f * width + e] = 1.0
    return (
        high, low,
        (np.cos(twist) * scale).astype(np.float32),
        (np.sin(twist) * scale).astype(np.float32),
        perm,
    )


def kernel_shards(echoes, guard_gates, train_gates):
    n = lax.axis_size("pulse")
    length, gates = echoes.shape[1], echoes.shape[2]
    chunks = CHUNKS if gates % (n * ROWS * CHUNKS) == 0 else 1
    part = gates // n // chunks
    smem = pl.BlockSpec(memory_space=pltpu.SMEM)
    vmem = pl.BlockSpec(memory_space=pltpu.VMEM)
    out = jax.ShapeDtypeStruct((length, gates), jnp.float32)
    dma = pltpu.SemaphoreType.DMA
    return pl.pallas_call(
        functools.partial(kernel, n, chunks),
        out_shape=(out, out),
        in_specs=[smem, smem] + [pl.BlockSpec(memory_space=pl.ANY)] * 6,
        out_specs=(vmem, vmem),
        scratch_shapes=[
            pltpu.VMEM((n, chunks, 2, part, length), jnp.float32),
            pltpu.VMEM((chunks, n, 2, part, length), jnp.float32),
            pltpu.VMEM((2, n, part, length), jnp.float32),
            pltpu.VMEM((n, chunks, part, length), jnp.float32),
            pltpu.VMEM((n, chunks, part, length), jnp.float32),
            pltpu.VMEM((length + 2 * ROWS, gates), jnp.float32),
            pltpu.VMEM((4, ROWS, gates), jnp.float32),
            pltpu.VMEM(echoes.shape, jnp.float32),
            pltpu.VMEM((length, 2 * length), jnp.bfloat16),
            pltpu.VMEM((length, 2 * length), jnp.bfloat16),
            pltpu.VMEM((n, length), jnp.float32),
            pltpu.VMEM((n, length), jnp.float32),
            pltpu.VMEM((length, length), jnp.float32),
            dma((chunks, n)), dma((chunks, n)), dma((chunks, n)), dma((chunks, n)),
            dma((2,)), dma((2,)), dma((7,)),
        ],
        compiler_params=pltpu.CompilerParams(
            collective_id=0, has_side_effects=True, vmem_limit_bytes=20 * 2**20
        ),
    )(guard_gates, train_gates, *(pltpu.with_memory_space_constraint(t, pltpu.HBM) for t in (echoes, *(jnp.asarray(t) for t in tables(n, length)))))


CHUNKS = 2


def shards(echoes, guard_gates, train_gates):
    n = lax.axis_size("pulse")
    length, gates = echoes.shape[1], echoes.shape[2]
    fits = length % LANES == 0 and length % n == 0 and n > 2 and gates % (n * ROWS) == 0
    fits = fits and n & (n - 1) == 0 and length & (length - 1) == 0 and LANES % (length // n) == 0
    if fits and GUARD_BINS + TRAIN_BINS <= ROWS:
        return kernel_shards(echoes, guard_gates, train_gates)
    return generic_shards(echoes, guard_gates, train_gates)


def solution(mesh):
    return jax.shard_map(
        shards,
        mesh=mesh,
        in_specs=(P(None, "pulse", "beam"), P(), P()),
        out_specs=(P("pulse", "beam"), P("pulse", "beam")),
        check_vma=False,
    )
```

```python
import functools

import jax
import jax.numpy as jnp
import numpy as np
from jax import lax
from jax.experimental import pallas as pl
from jax.experimental.pallas import tpu as pltpu
from jax.sharding import PartitionSpec as P

PULSES = 4096
GUARD_BINS = 2
TRAIN_BINS = 4


TWO_PI = 6.283185307179586


def padded_2(cells, sides, width):
    for axis, dim in sides:
        count = lax.axis_size(axis)
        head = lax.slice_in_dim(cells, 0, width, axis=dim)
        tail = lax.slice_in_dim(cells, cells.shape[dim] - width, cells.shape[dim], axis=dim)
        cells = jnp.concatenate(
            [
                lax.ppermute(tail, axis, [(i, (i + 1) % count) for i in range(count)]),
                cells,
                lax.ppermute(head, axis, [((i + 1) % count, i) for i in range(count)]),
            ],
            axis=dim,
        )
    return cells


def small_tables(count):
    index_row = jnp.arange(count, dtype=jnp.int32)
    phases = (index_row[:, None] * index_row[None, :] % count).astype(jnp.float32) * (
        TWO_PI / count
    )
    return (jnp.cos(phases), jnp.sin(phases))


def product(left, right):
    return jnp.dot(left, right, precision=lax.Precision.HIGHEST, preferred_element_type=jnp.float32)


def factored_powers(samples):
    width = samples.shape[2]
    bit_count = PULSES.bit_length() - 1
    first_radix = 2 ** (bit_count // 2)
    second_radix = PULSES // first_radix
    cos_first, sin_first = small_tables(first_radix)
    real_in = samples[0].reshape(first_radix, second_radix * width)
    imag_in = samples[1].reshape(first_radix, second_radix * width)
    real_one = (product(cos_first, real_in) + product(sin_first, imag_in)).reshape(
        first_radix, second_radix, width
    )
    imag_one = (product(cos_first, imag_in) - product(sin_first, real_in)).reshape(
        first_radix, second_radix, width
    )
    first_ids = jnp.arange(first_radix, dtype=jnp.int32)
    second_ids = jnp.arange(second_radix, dtype=jnp.int32)
    twist = (first_ids[:, None] * second_ids[None, :] % PULSES).astype(jnp.float32) * (
        TWO_PI / PULSES
    )
    twist_cos = jnp.cos(twist)[:, :, None]
    twist_sin = jnp.sin(twist)[:, :, None]
    real_two = twist_cos * real_one + twist_sin * imag_one
    imag_two = twist_cos * imag_one - twist_sin * real_one
    real_two = jnp.transpose(real_two, (1, 0, 2)).reshape(second_radix, first_radix * width)
    imag_two = jnp.transpose(imag_two, (1, 0, 2)).reshape(second_radix, first_radix * width)
    cos_second, sin_second = small_tables(second_radix)
    scale_factor = 1.0 / jnp.sqrt(jnp.float32(PULSES))
    real_out = (product(cos_second, real_two) + product(sin_second, imag_two)) * scale_factor
    imag_out = (product(cos_second, imag_two) - product(sin_second, real_two)) * scale_factor
    result = real_out * real_out + imag_out * imag_out
    return result.reshape(PULSES, width)


def generic_shards(echoes, guard_gates, train_gates):
    devices_count = lax.axis_size("pulse")
    bins_local = PULSES // devices_count
    gates_count = echoes.shape[2]
    columns = factored_powers(
        lax.all_to_all(echoes, "pulse", split_axis=2, concat_axis=1, tiled=True)
    )
    powers = lax.all_to_all(columns, "pulse", split_axis=0, concat_axis=1, tiled=True)
    reach = GUARD_BINS + TRAIN_BINS
    padded = padded_2(powers, (("pulse", 0),), reach)
    doppler_sum = jnp.zeros_like(powers)
    for shift_bins in range(GUARD_BINS + 1, reach + 1):
        above = padded[reach + shift_bins : reach + shift_bins + bins_local]
        below = padded[reach - shift_bins : reach - shift_bins + bins_local]
        doppler_sum = doppler_sum + above + below
    guard_width = guard_gates[0]
    train_width = train_gates[0]
    gate_ids = jnp.arange(gates_count, dtype=jnp.int32)
    offsets = jnp.abs(gate_ids[:, None] - gate_ids[None, :])
    band = ((offsets > guard_width) & (offsets <= guard_width + train_width)).astype(jnp.float32)
    range_sum = jnp.dot(
        powers, band, precision=lax.Precision.HIGHEST, preferred_element_type=jnp.float32
    )
    range_count = jnp.sum(band, axis=0)
    noise_level = (range_sum + doppler_sum) / (range_count[None, :] + 2.0 * TRAIN_BINS)
    statistic = powers / (noise_level + 1.0)
    return (powers, statistic)


LANES = 128
ROWS = 8
HIGHEST = lax.Precision.HIGHEST


def butterflies(cells):
    count = len(cells)
    if count == 1:
        return cells
    even = butterflies(cells[0::2])
    odd = butterflies(cells[1::2])
    low, high = [], []
    for k in range(count // 2):
        re, im = odd[k]
        if 4 * k == count:
            re, im = im, -re
        elif k:
            c, s = np.cos(2 * np.pi * k / count), np.sin(2 * np.pi * k / count)
            c, s = np.float32(c), np.float32(s)
            re, im = c * re + s * im, c * im - s * re
        low.append((even[k][0] + re, even[k][1] + im))
        high.append((even[k][0] - re, even[k][1] - im))
    return low + high


def swap_digits(rows, width):
    count = len(rows)
    lane = lax.broadcasted_iota(jnp.int32, rows[0][0].shape, 1)
    bit = 1
    while bit < count:
        step = bit * width
        keep = (lane // step) % 2 == 0 if step < LANES else None
        for f in range(count):
            if f & bit:
                continue
            first, second = rows[f], rows[f | bit]
            if step < LANES:
                new_first = [
                    jnp.where(keep, a, pltpu.roll(b, step, 1)) for a, b in zip(first, second)
                ]
                new_second = [
                    jnp.where(keep, pltpu.roll(a, LANES - step, 1), b)
                    for a, b in zip(first, second)
                ]
            else:
                hop = step // LANES
                new_first, new_second = list(first), list(second)
                for h in range(len(first)):
                    if h & hop:
                        new_first[h] = second[h ^ hop]
                    else:
                        new_second[h] = first[h ^ hop]
            rows[f], rows[f | bit] = new_first, new_second
        bit *= 2
    return rows


def split(values):
    high = values.astype(jnp.bfloat16)
    return high, (values - high.astype(jnp.float32)).astype(jnp.bfloat16)


def bf16_dot(left, right, dims=(((1,), (0,)), ((), ()))):
    return lax.dot_general(left, right, dims, preferred_element_type=jnp.float32)


def rows_of(picks, columns):
    return lax.dot_general(
        picks, columns, (((1,), (1,)), ((), ())),
        precision=HIGHEST, preferred_element_type=jnp.float32,
    )


def kernel(
    n, chunks, guard_ref, train_ref, x_any, high_any, low_any, cos_any, sin_any, perm_any,
    power_ref, stat_ref,
    sent, got, mixed, cells, landed, padded, edges,
    x_ref, table_high, table_low, twist_cos, twist_sin, perm_ref,
    send_one, recv_one, send_two, recv_two, send_edge, recv_edge, load,
):
    me = lax.axis_index("pulse")
    length, gates = x_ref.shape[1], x_ref.shape[2]
    part = gates // n // chunks
    halves = length // LANES
    barrier = pltpu.get_barrier_semaphore()
    for o in peer_order(n):
        pl.semaphore_signal(barrier, inc=1, device_id={"pulse": partner(me, o)})
    loads = [pltpu.make_async_copy(x_any.at[p], x_ref.at[p], load.at[p]) for p in range(2)]
    pairs = (
        (high_any, table_high), (low_any, table_low), (cos_any, twist_cos), (sin_any, twist_sin),
        (perm_any, perm_ref),
    )
    for i, (source, target) in enumerate(pairs):
        loads.append(pltpu.make_async_copy(source, target, load.at[2 + i]))
    for copy in loads:
        copy.start()
    for p in range(2):
        loads[p].wait()
        sent[:, :, p] = x_ref[p].T.reshape(n, chunks, part, length)
    pl.semaphore_wait(barrier, n - 1)

    def first_copy(c, o):
        peer = partner(me, o)
        return pltpu.make_async_remote_copy(
            src_ref=sent.at[peer, c], dst_ref=got.at[c, me],
            send_sem=send_one.at[c, o], recv_sem=recv_one.at[c, o],
            device_id={"pulse": peer},
        )

    def second_copy(c, o):
        peer = partner(me, o)
        return pltpu.make_async_remote_copy(
            src_ref=cells.at[peer, c], dst_ref=landed.at[me, c],
            send_sem=send_two.at[c, o], recv_sem=recv_two.at[c, o],
            device_id={"pulse": peer},
        )

    order = peer_order(n)
    for c in range(chunks):
        for o in order:
            first_copy(c, o).start()
    for c in range(chunks):
        got[c, me] = sent[me, c]
    for copy in loads[2:]:
        copy.wait()
    gate_row = lax.broadcasted_iota(jnp.int32, (gates, gates), 0)
    gate_col = lax.broadcasted_iota(jnp.int32, (gates, gates), 1)
    offsets = jnp.abs(gate_row - gate_col)
    guard, train = guard_ref[0], train_ref[0]
    inside = ((offsets > guard) & (offsets <= guard + train)).astype(jnp.float32)
    range_count = jnp.sum(inside, axis=0, keepdims=True)
    band = inside.astype(jnp.bfloat16)

    for c in range(chunks):
        for o in order:
            first_copy(c, o).wait_recv()
        for r in range(0, part, ROWS):
            for h in range(halves):
                lanes = slice(h * LANES, (h + 1) * LANES)
                spectra = butterflies(
                    [
                        (got[c, s, 0, r : r + ROWS, lanes], got[c, s, 1, r : r + ROWS, lanes])
                        for s in range(n)
                    ]
                )
                for f, (re, im) in enumerate(spectra):
                    tc, ts = twist_cos[f : f + 1, lanes], twist_sin[f : f + 1, lanes]
                    mixed[0, f, r : r + ROWS, lanes] = tc * re + ts * im
                    mixed[1, f, r : r + ROWS, lanes] = tc * im - ts * re
        high, low = split(mixed[...].reshape(2 * n * part, length))
        both = (
            bf16_dot(high, table_high[...])
            + bf16_dot(low, table_high[...])
            + bf16_dot(high, table_low[...])
        ).reshape(2, n * part, 2 * length)
        real = both[0, :, :length] + both[1, :, length:]
        imag = both[1, :, :length] - both[0, :, length:]
        power = (real * real + imag * imag).reshape(n, part, length)
        rows = [
            [power[f, :, h * LANES : (h + 1) * LANES] for h in range(halves)] for f in range(n)
        ]
        rows = swap_digits(rows, length // n)
        for d in range(n):
            for h in range(halves):
                cells[d, c, :, h * LANES : (h + 1) * LANES] = rows[d][h]
        for o in order:
            second_copy(c, o).start()
        landed[me, c] = cells[me, c]
    for c in range(chunks):
        for o in order:
            second_copy(c, o).wait_recv()

    columns = landed[...].reshape(gates, length)
    ends = jnp.concatenate([perm_ref[:ROWS], perm_ref[length - ROWS :]])
    ends = rows_of(ends, columns)
    edges[0] = ends[:ROWS]
    edges[1] = ends[ROWS:]
    above, below = lax.rem(me + 1, n), lax.rem(me + n - 1, n)
    tail_copy = pltpu.make_async_remote_copy(
        src_ref=edges.at[1], dst_ref=edges.at[2],
        send_sem=send_edge.at[0], recv_sem=recv_edge.at[0], device_id={"pulse": above},
    )
    head_copy = pltpu.make_async_remote_copy(
        src_ref=edges.at[0], dst_ref=edges.at[3],
        send_sem=send_edge.at[1], recv_sem=recv_edge.at[1], device_id={"pulse": below},
    )
    tail_copy.start()
    head_copy.start()
    powers = rows_of(perm_ref[...], columns)
    power_ref[...] = powers
    high, low = split(powers)
    range_sum = bf16_dot(high, band) + bf16_dot(low, band)
    padded[ROWS : ROWS + length] = powers

    def finish(first, last):
        total = range_sum[first:last]
        for d in range(GUARD_BINS + 1, GUARD_BINS + TRAIN_BINS + 1):
            for move in (d, -d):
                total = total + padded[ROWS + first + move : ROWS + last + move]
        noise = total / (range_count + 2.0 * TRAIN_BINS)
        stat_ref[first:last] = powers[first:last] / (noise + 1.0)

    finish(ROWS, length - ROWS)
    tail_copy.wait_recv()
    head_copy.wait_recv()
    padded[:ROWS] = edges[2]
    padded[ROWS + length :] = edges[3]
    finish(0, ROWS)
    finish(length - ROWS, length)
    tail_copy.wait_send()
    head_copy.wait_send()
    for c in range(chunks):
        for o in order:
            first_copy(c, o).wait_send()
            second_copy(c, o).wait_send()


def partner(me, offset):
    peer, bit = me, 1
    while bit <= offset:
        if offset & bit:
            peer = peer + bit * (1 - 2 * lax.rem(lax.div(me, bit), 2))
        bit *= 2
    return peer


def peer_order(n):
    return list(range(n - 1, 0, -1))


def tables(n, length):
    lane = np.arange(length)
    turn = 2 * np.pi * (np.outer(lane, lane) % length) / length
    both = np.concatenate([np.cos(turn), np.sin(turn)], axis=1).astype(np.float32)
    high = both.astype(jnp.bfloat16)
    low = (both - high.astype(np.float32)).astype(jnp.bfloat16)
    twist = 2 * np.pi * np.outer(np.arange(n), lane) / (n * length)
    scale = 1.0 / np.sqrt(n * length)
    perm = np.zeros((length, length), np.float32)
    width = length // n
    for f in range(n):
        for e in range(width):
            perm[f + n * e, f * width + e] = 1.0
    return (
        high, low,
        (np.cos(twist) * scale).astype(np.float32),
        (np.sin(twist) * scale).astype(np.float32),
        perm,
    )


def kernel_shards(echoes, guard_gates, train_gates):
    n = lax.axis_size("pulse")
    length, gates = echoes.shape[1], echoes.shape[2]
    chunks = CHUNKS if gates % (n * ROWS * CHUNKS) == 0 else 1
    part = gates // n // chunks
    smem = pl.BlockSpec(memory_space=pltpu.SMEM)
    vmem = pl.BlockSpec(memory_space=pltpu.VMEM)
    out = jax.ShapeDtypeStruct((length, gates), jnp.float32)
    dma = pltpu.SemaphoreType.DMA
    results = pl.pallas_call(
        functools.partial(kernel, n, chunks),
        out_shape=(out, out),
        in_specs=[smem, smem] + [pl.BlockSpec(memory_space=pl.ANY)] * 6,
        out_specs=(vmem, vmem),
        scratch_shapes=[
            pltpu.VMEM((n, chunks, 2, part, length), jnp.float32),
            pltpu.VMEM((chunks, n, 2, part, length), jnp.float32),
            pltpu.VMEM((2, n, part, length), jnp.float32),
            pltpu.VMEM((n, chunks, part, length), jnp.float32),
            pltpu.VMEM((n, chunks, part, length), jnp.float32),
            pltpu.VMEM((length + 2 * ROWS, gates), jnp.float32),
            pltpu.VMEM((4, ROWS, gates), jnp.float32),
            pltpu.VMEM(echoes.shape, jnp.float32),
            pltpu.VMEM((length, 2 * length), jnp.bfloat16),
            pltpu.VMEM((length, 2 * length), jnp.bfloat16),
            pltpu.VMEM((n, length), jnp.float32),
            pltpu.VMEM((n, length), jnp.float32),
            pltpu.VMEM((length, length), jnp.float32),
            dma((chunks, n)), dma((chunks, n)), dma((chunks, n)), dma((chunks, n)),
            dma((2,)), dma((2,)), dma((7,)),
        ],
        compiler_params=pltpu.CompilerParams(
            collective_id=0, has_side_effects=True, vmem_limit_bytes=20 * 2**20
        ),
    )(guard_gates, train_gates, *(pltpu.with_memory_space_constraint(t, pltpu.HBM) for t in (echoes, *(jnp.asarray(t) for t in tables(n, length)))))
    return pl.pallas_call(
        write_out,
        out_shape=(out, out),
        in_specs=[vmem] * 2,
        out_specs=(pl.BlockSpec(memory_space=pl.ANY),) * 2,
        scratch_shapes=[dma((2,))],
        compiler_params=pltpu.CompilerParams(vmem_limit_bytes=8 * 2**20),
    )(*results)


def write_out(power_in, stat_in, power_out, stat_out, done):
    copies = [
        pltpu.make_async_copy(power_in, power_out, done.at[0]),
        pltpu.make_async_copy(stat_in, stat_out, done.at[1]),
    ]
    for copy in copies:
        copy.start()
    for copy in copies:
        copy.wait()


CHUNKS = 2


def shards(echoes, guard_gates, train_gates):
    n = lax.axis_size("pulse")
    length, gates = echoes.shape[1], echoes.shape[2]
    fits = length % LANES == 0 and length % n == 0 and n > 2 and gates % (n * ROWS) == 0
    fits = fits and n & (n - 1) == 0 and length & (length - 1) == 0 and LANES % (length // n) == 0
    if fits and GUARD_BINS + TRAIN_BINS <= ROWS:
        return kernel_shards(echoes, guard_gates, train_gates)
    return generic_shards(echoes, guard_gates, train_gates)


def solution(mesh):
    return jax.shard_map(
        shards,
        mesh=mesh,
        in_specs=(P(None, "pulse", "beam"), P(), P()),
        out_specs=(P("pulse", "beam"), P("pulse", "beam")),
        check_vma=False,
    )
```

```python
import functools

import jax
import jax.numpy as jnp
import numpy as np
from jax import lax
from jax.experimental import pallas as pl
from jax.experimental.pallas import tpu as pltpu
from jax.sharding import PartitionSpec as P

PULSES = 4096
GUARD_BINS = 2
TRAIN_BINS = 4


TWO_PI = 6.283185307179586


def padded_2(cells, sides, width):
    for axis, dim in sides:
        count = lax.axis_size(axis)
        head = lax.slice_in_dim(cells, 0, width, axis=dim)
        tail = lax.slice_in_dim(cells, cells.shape[dim] - width, cells.shape[dim], axis=dim)
        cells = jnp.concatenate(
            [
                lax.ppermute(tail, axis, [(i, (i + 1) % count) for i in range(count)]),
                cells,
                lax.ppermute(head, axis, [((i + 1) % count, i) for i in range(count)]),
            ],
            axis=dim,
        )
    return cells


def small_tables(count):
    index_row = jnp.arange(count, dtype=jnp.int32)
    phases = (index_row[:, None] * index_row[None, :] % count).astype(jnp.float32) * (
        TWO_PI / count
    )
    return (jnp.cos(phases), jnp.sin(phases))


def product(left, right):
    return jnp.dot(left, right, precision=lax.Precision.HIGHEST, preferred_element_type=jnp.float32)


def factored_powers(samples):
    width = samples.shape[2]
    bit_count = PULSES.bit_length() - 1
    first_radix = 2 ** (bit_count // 2)
    second_radix = PULSES // first_radix
    cos_first, sin_first = small_tables(first_radix)
    real_in = samples[0].reshape(first_radix, second_radix * width)
    imag_in = samples[1].reshape(first_radix, second_radix * width)
    real_one = (product(cos_first, real_in) + product(sin_first, imag_in)).reshape(
        first_radix, second_radix, width
    )
    imag_one = (product(cos_first, imag_in) - product(sin_first, real_in)).reshape(
        first_radix, second_radix, width
    )
    first_ids = jnp.arange(first_radix, dtype=jnp.int32)
    second_ids = jnp.arange(second_radix, dtype=jnp.int32)
    twist = (first_ids[:, None] * second_ids[None, :] % PULSES).astype(jnp.float32) * (
        TWO_PI / PULSES
    )
    twist_cos = jnp.cos(twist)[:, :, None]
    twist_sin = jnp.sin(twist)[:, :, None]
    real_two = twist_cos * real_one + twist_sin * imag_one
    imag_two = twist_cos * imag_one - twist_sin * real_one
    real_two = jnp.transpose(real_two, (1, 0, 2)).reshape(second_radix, first_radix * width)
    imag_two = jnp.transpose(imag_two, (1, 0, 2)).reshape(second_radix, first_radix * width)
    cos_second, sin_second = small_tables(second_radix)
    scale_factor = 1.0 / jnp.sqrt(jnp.float32(PULSES))
    real_out = (product(cos_second, real_two) + product(sin_second, imag_two)) * scale_factor
    imag_out = (product(cos_second, imag_two) - product(sin_second, real_two)) * scale_factor
    result = real_out * real_out + imag_out * imag_out
    return result.reshape(PULSES, width)


def generic_shards(echoes, guard_gates, train_gates):
    devices_count = lax.axis_size("pulse")
    bins_local = PULSES // devices_count
    gates_count = echoes.shape[2]
    columns = factored_powers(
        lax.all_to_all(echoes, "pulse", split_axis=2, concat_axis=1, tiled=True)
    )
    powers = lax.all_to_all(columns, "pulse", split_axis=0, concat_axis=1, tiled=True)
    reach = GUARD_BINS + TRAIN_BINS
    padded = padded_2(powers, (("pulse", 0),), reach)
    doppler_sum = jnp.zeros_like(powers)
    for shift_bins in range(GUARD_BINS + 1, reach + 1):
        above = padded[reach + shift_bins : reach + shift_bins + bins_local]
        below = padded[reach - shift_bins : reach - shift_bins + bins_local]
        doppler_sum = doppler_sum + above + below
    guard_width = guard_gates[0]
    train_width = train_gates[0]
    gate_ids = jnp.arange(gates_count, dtype=jnp.int32)
    offsets = jnp.abs(gate_ids[:, None] - gate_ids[None, :])
    band = ((offsets > guard_width) & (offsets <= guard_width + train_width)).astype(jnp.float32)
    range_sum = jnp.dot(
        powers, band, precision=lax.Precision.HIGHEST, preferred_element_type=jnp.float32
    )
    range_count = jnp.sum(band, axis=0)
    noise_level = (range_sum + doppler_sum) / (range_count[None, :] + 2.0 * TRAIN_BINS)
    statistic = powers / (noise_level + 1.0)
    return (powers, statistic)


LANES = 128
ROWS = 8
HIGHEST = lax.Precision.HIGHEST


def butterflies(cells):
    count = len(cells)
    if count == 1:
        return cells
    even = butterflies(cells[0::2])
    odd = butterflies(cells[1::2])
    low, high = [], []
    for k in range(count // 2):
        re, im = odd[k]
        if 4 * k == count:
            re, im = im, -re
        elif k:
            c, s = np.cos(2 * np.pi * k / count), np.sin(2 * np.pi * k / count)
            c, s = np.float32(c), np.float32(s)
            re, im = c * re + s * im, c * im - s * re
        low.append((even[k][0] + re, even[k][1] + im))
        high.append((even[k][0] - re, even[k][1] - im))
    return low + high


def swap_digits(rows, width):
    count = len(rows)
    lane = lax.broadcasted_iota(jnp.int32, rows[0][0].shape, 1)
    bit = 1
    while bit < count:
        step = bit * width
        keep = (lane // step) % 2 == 0 if step < LANES else None
        for f in range(count):
            if f & bit:
                continue
            first, second = rows[f], rows[f | bit]
            if step < LANES:
                new_first = [
                    jnp.where(keep, a, pltpu.roll(b, step, 1)) for a, b in zip(first, second)
                ]
                new_second = [
                    jnp.where(keep, pltpu.roll(a, LANES - step, 1), b)
                    for a, b in zip(first, second)
                ]
            else:
                hop = step // LANES
                new_first, new_second = list(first), list(second)
                for h in range(len(first)):
                    if h & hop:
                        new_first[h] = second[h ^ hop]
                    else:
                        new_second[h] = first[h ^ hop]
            rows[f], rows[f | bit] = new_first, new_second
        bit *= 2
    return rows


def split(values):
    high = values.astype(jnp.bfloat16)
    return high, (values - high.astype(jnp.float32)).astype(jnp.bfloat16)


def bf16_dot(left, right, dims=(((1,), (0,)), ((), ()))):
    return lax.dot_general(left, right, dims, preferred_element_type=jnp.float32)


def rows_of(picks, columns):
    return lax.dot_general(
        picks, columns, (((1,), (1,)), ((), ())),
        precision=HIGHEST, preferred_element_type=jnp.float32,
    )


def kernel(
    n, chunks, guard_ref, train_ref, x_any, high_any, low_any, cos_any, sin_any, perm_any,
    power_ref, stat_ref,
    sent, got, mixed, cells, landed, padded, edges,
    x_ref, table_high, table_low, twist_cos, twist_sin, perm_ref,
    send_one, recv_one, send_two, recv_two, send_edge, recv_edge, load,
):
    me = lax.axis_index("pulse")
    length, gates = x_ref.shape[1], x_ref.shape[2]
    part = gates // n // chunks
    halves = length // LANES
    barrier = pltpu.get_barrier_semaphore()
    for o in peer_order(n):
        pl.semaphore_signal(barrier, inc=1, device_id={"pulse": partner(me, o)})
    loads = [pltpu.make_async_copy(x_any.at[p], x_ref.at[p], load.at[p]) for p in range(2)]
    pairs = (
        (high_any, table_high), (low_any, table_low), (cos_any, twist_cos), (sin_any, twist_sin),
        (perm_any, perm_ref),
    )
    for i, (source, target) in enumerate(pairs):
        loads.append(pltpu.make_async_copy(source, target, load.at[2 + i]))
    for copy in loads:
        copy.start()
    for p in range(2):
        loads[p].wait()
        sent[:, :, p] = x_ref[p].T.reshape(n, chunks, part, length)
    pl.semaphore_wait(barrier, n - 1)

    def first_copy(c, o):
        peer = partner(me, o)
        return pltpu.make_async_remote_copy(
            src_ref=sent.at[peer, c], dst_ref=got.at[c, me],
            send_sem=send_one.at[c, o], recv_sem=recv_one.at[c, o],
            device_id={"pulse": peer},
        )

    def second_copy(c, o):
        peer = partner(me, o)
        return pltpu.make_async_remote_copy(
            src_ref=cells.at[peer, c], dst_ref=landed.at[me, c],
            send_sem=send_two.at[c, o], recv_sem=recv_two.at[c, o],
            device_id={"pulse": peer},
        )

    order = peer_order(n)
    for c in range(chunks):
        for o in order:
            first_copy(c, o).start()
    for c in range(chunks):
        got[c, me] = sent[me, c]
    for copy in loads[2:]:
        copy.wait()
    gate_row = lax.broadcasted_iota(jnp.int32, (gates, gates), 0)
    gate_col = lax.broadcasted_iota(jnp.int32, (gates, gates), 1)
    offsets = jnp.abs(gate_row - gate_col)
    guard, train = guard_ref[0], train_ref[0]
    inside = ((offsets > guard) & (offsets <= guard + train)).astype(jnp.float32)
    range_count = jnp.sum(inside, axis=0, keepdims=True)
    band = inside.astype(jnp.bfloat16)

    for c in range(chunks):
        for o in order:
            first_copy(c, o).wait_recv()
        for r in range(0, part, ROWS):
            for h in range(halves):
                lanes = slice(h * LANES, (h + 1) * LANES)
                spectra = butterflies(
                    [
                        (got[c, s, 0, r : r + ROWS, lanes], got[c, s, 1, r : r + ROWS, lanes])
                        for s in range(n)
                    ]
                )
                for f, (re, im) in enumerate(spectra):
                    tc, ts = twist_cos[f : f + 1, lanes], twist_sin[f : f + 1, lanes]
                    mixed[0, f, r : r + ROWS, lanes] = tc * re + ts * im
                    mixed[1, f, r : r + ROWS, lanes] = tc * im - ts * re
        high, low = split(mixed[...].reshape(2 * n * part, length))
        both = (
            bf16_dot(high, table_high[...])
            + bf16_dot(low, table_high[...])
            + bf16_dot(high, table_low[...])
        ).reshape(2, n * part, 2 * length)
        real = both[0, :, :length] + both[1, :, length:]
        imag = both[1, :, :length] - both[0, :, length:]
        power = (real * real + imag * imag).reshape(n, part, length)
        rows = [
            [power[f, :, h * LANES : (h + 1) * LANES] for h in range(halves)] for f in range(n)
        ]
        rows = swap_digits(rows, length // n)
        for d in range(n):
            for h in range(halves):
                cells[d, c, :, h * LANES : (h + 1) * LANES] = rows[d][h]
        for o in order:
            second_copy(c, o).start()
        landed[me, c] = cells[me, c]
    for c in range(chunks):
        for o in order:
            second_copy(c, o).wait_recv()

    columns = landed[...].reshape(gates, length)
    ends = jnp.concatenate([perm_ref[:ROWS], perm_ref[length - ROWS :]])
    ends = rows_of(ends, columns)
    edges[0] = ends[:ROWS]
    edges[1] = ends[ROWS:]
    above, below = lax.rem(me + 1, n), lax.rem(me + n - 1, n)
    tail_copy = pltpu.make_async_remote_copy(
        src_ref=edges.at[1], dst_ref=edges.at[2],
        send_sem=send_edge.at[0], recv_sem=recv_edge.at[0], device_id={"pulse": above},
    )
    head_copy = pltpu.make_async_remote_copy(
        src_ref=edges.at[0], dst_ref=edges.at[3],
        send_sem=send_edge.at[1], recv_sem=recv_edge.at[1], device_id={"pulse": below},
    )
    tail_copy.start()
    head_copy.start()
    powers = rows_of(perm_ref[...], columns)
    power_ref[...] = powers
    high, low = split(powers)
    range_sum = bf16_dot(high, band) + bf16_dot(low, band)
    padded[ROWS : ROWS + length] = powers

    def finish(first, last):
        total = range_sum[first:last]
        for d in range(GUARD_BINS + 1, GUARD_BINS + TRAIN_BINS + 1):
            for move in (d, -d):
                total = total + padded[ROWS + first + move : ROWS + last + move]
        noise = total / (range_count + 2.0 * TRAIN_BINS)
        stat_ref[first:last] = powers[first:last] / (noise + 1.0)

    finish(ROWS, length - ROWS)
    tail_copy.wait_recv()
    head_copy.wait_recv()
    padded[:ROWS] = edges[2]
    padded[ROWS + length :] = edges[3]
    finish(0, ROWS)
    finish(length - ROWS, length)
    tail_copy.wait_send()
    head_copy.wait_send()
    for c in range(chunks):
        for o in order:
            first_copy(c, o).wait_send()
            second_copy(c, o).wait_send()


def partner(me, offset):
    peer, bit = me, 1
    while bit <= offset:
        if offset & bit:
            peer = peer + bit * (1 - 2 * lax.rem(lax.div(me, bit), 2))
        bit *= 2
    return peer


def peer_order(n):
    half, quarter = n // 2, n // 4
    near, far = range(half - 1, quarter - 1, -1), range(n - 1, half - 1, -1)
    return [*near, *far, *range(quarter - 1, 0, -1)]


def tables(n, length):
    lane = np.arange(length)
    turn = 2 * np.pi * (np.outer(lane, lane) % length) / length
    both = np.concatenate([np.cos(turn), np.sin(turn)], axis=1).astype(np.float32)
    high = both.astype(jnp.bfloat16)
    low = (both - high.astype(np.float32)).astype(jnp.bfloat16)
    twist = 2 * np.pi * np.outer(np.arange(n), lane) / (n * length)
    scale = 1.0 / np.sqrt(n * length)
    perm = np.zeros((length, length), np.float32)
    width = length // n
    for f in range(n):
        for e in range(width):
            perm[f + n * e, f * width + e] = 1.0
    return (
        high, low,
        (np.cos(twist) * scale).astype(np.float32),
        (np.sin(twist) * scale).astype(np.float32),
        perm,
    )


def kernel_shards(echoes, guard_gates, train_gates):
    n = lax.axis_size("pulse")
    length, gates = echoes.shape[1], echoes.shape[2]
    chunks = CHUNKS if gates % (n * ROWS * CHUNKS) == 0 else 1
    part = gates // n // chunks
    smem = pl.BlockSpec(memory_space=pltpu.SMEM)
    vmem = pl.BlockSpec(memory_space=pltpu.VMEM)
    out = jax.ShapeDtypeStruct((length, gates), jnp.float32)
    dma = pltpu.SemaphoreType.DMA
    results = pl.pallas_call(
        functools.partial(kernel, n, chunks),
        out_shape=(out, out),
        in_specs=[smem, smem] + [pl.BlockSpec(memory_space=pl.ANY)] * 6,
        out_specs=(vmem, vmem),
        scratch_shapes=[
            pltpu.VMEM((n, chunks, 2, part, length), jnp.float32),
            pltpu.VMEM((chunks, n, 2, part, length), jnp.float32),
            pltpu.VMEM((2, n, part, length), jnp.float32),
            pltpu.VMEM((n, chunks, part, length), jnp.float32),
            pltpu.VMEM((n, chunks, part, length), jnp.float32),
            pltpu.VMEM((length + 2 * ROWS, gates), jnp.float32),
            pltpu.VMEM((4, ROWS, gates), jnp.float32),
            pltpu.VMEM(echoes.shape, jnp.float32),
            pltpu.VMEM((length, 2 * length), jnp.bfloat16),
            pltpu.VMEM((length, 2 * length), jnp.bfloat16),
            pltpu.VMEM((n, length), jnp.float32),
            pltpu.VMEM((n, length), jnp.float32),
            pltpu.VMEM((length, length), jnp.float32),
            dma((chunks, n)), dma((chunks, n)), dma((chunks, n)), dma((chunks, n)),
            dma((2,)), dma((2,)), dma((7,)),
        ],
        compiler_params=pltpu.CompilerParams(
            collective_id=0, has_side_effects=True, vmem_limit_bytes=20 * 2**20
        ),
    )(guard_gates, train_gates, *(pltpu.with_memory_space_constraint(t, pltpu.HBM) for t in (echoes, *(jnp.asarray(t) for t in tables(n, length)))))
    return pl.pallas_call(
        write_out,
        out_shape=(out, out),
        in_specs=[vmem] * 2,
        out_specs=(pl.BlockSpec(memory_space=pl.ANY),) * 2,
        scratch_shapes=[dma((2,))],
        compiler_params=pltpu.CompilerParams(vmem_limit_bytes=8 * 2**20),
    )(*results)


def write_out(power_in, stat_in, power_out, stat_out, done):
    copies = [
        pltpu.make_async_copy(power_in, power_out, done.at[0]),
        pltpu.make_async_copy(stat_in, stat_out, done.at[1]),
    ]
    for copy in copies:
        copy.start()
    for copy in copies:
        copy.wait()


CHUNKS = 2


def shards(echoes, guard_gates, train_gates):
    n = lax.axis_size("pulse")
    length, gates = echoes.shape[1], echoes.shape[2]
    fits = length % LANES == 0 and length % n == 0 and n > 2 and gates % (n * ROWS) == 0
    fits = fits and n & (n - 1) == 0 and length & (length - 1) == 0 and LANES % (length // n) == 0
    if fits and GUARD_BINS + TRAIN_BINS <= ROWS:
        return kernel_shards(echoes, guard_gates, train_gates)
    return generic_shards(echoes, guard_gates, train_gates)


def solution(mesh):
    return jax.shard_map(
        shards,
        mesh=mesh,
        in_specs=(P(None, "pulse", "beam"), P(), P()),
        out_specs=(P("pulse", "beam"), P("pulse", "beam")),
        check_vma=False,
    )
```
